256 devices in a mesh: row: 8 (over y, core), col: 4 (over x), layer: 8 (over z).
Axes of the slice: x: 4, y: 4, z: 8, core: 2. Of those that a mesh axis runs over, the one named last changes fastest.
Arguments:
- hamiltonian: bfloat16 [5120, 5120], P(('row', 'layer'), 'col'), may hold values from -1.2 to 1.2, as said below
- tile_pattern: int32 [40, 40], replicated, may hold values from 0 to 1, as said below
- n_occ: int32 [1], replicated, may hold values from 1024 to 4095
- mu: float32 [1], replicated, may hold values from -0.2 to 0.2
- gamma: float32 [1], replicated, may hold values from 0.25 to 0.4
Outputs:
- density: float32 [5120, 5120], P(('row', 'layer'), 'col')
The draws below stay inside these ranges and needn't reach their ends.
Inputs may be any that keep to these rules, and one draw needn't show every extreme that they name: `tile_pattern`: Symmetric, 0 or 1, with ones on the diagonal and next to it. `hamiltonian`: Symmetric; its eigenvalues lie within -1.8 and 1.8.
All inputs are finite; a program needn't handle non-finite values.
Results may differ from the reference program's by a relative error of at most 0.0055.
Values may be sent and summed in bfloat16 or wider, within the bound.
No kernel may reach another device: no remote copies, remote signals or barrier semaphores. Data moves between devices by JAX's collectives and lax.ppermute only.
A program may use at most 64 MiB of HBM per device.

```python
import jax
import jax.numpy as jnp

TILE = 128
STEPS = 2
TILES = 40
NORB = 5120


def tile_layout(key):
    row_ids = jnp.arange(TILES, dtype=jnp.int32)[:, None]
    col_ids = jnp.arange(TILES, dtype=jnp.int32)[None, :]
    tile_score = jax.random.randint(key, (TILES, TILES), 0, 100, dtype=jnp.int32)
    tile_score = jnp.where(row_ids <= col_ids, tile_score, tile_score.T)
    chance = 3 + 30 * (row_ids + col_ids) // (2 * TILES)
    near_diag = jnp.abs(row_ids - col_ids) <= 1
    return jnp.where(near_diag | (tile_score < chance), 1, 0).astype(jnp.int32)


def draw_tile_pattern(key, part):
    return tile_layout(jax.random.fold_in(key, 7))


def draw_hamiltonian(key, part):
    pattern = tile_layout(jax.random.fold_in(key, 7))
    dense_mask = jnp.repeat(jnp.repeat(pattern, TILE, 0), TILE, 1).astype(jnp.float32)
    row_count = jnp.sum(dense_mask, axis=1)
    row_weight = row_count ** (-0.25)
    first_key, second_key = jax.random.split(jax.random.fold_in(key, 13))
    noise_field = jax.random.normal(first_key, (NORB, NORB), jnp.float32)
    onsite = jax.random.uniform(second_key, (NORB,), jnp.float32, -0.2, 0.2)
    noise_field = jnp.clip((noise_field + noise_field.T) * 0.7071, -4.0, 4.0)
    identity = jnp.eye(NORB, dtype=jnp.float32)
    scaling = 0.65 * row_weight[:, None] * row_weight[None, :]
    coupled = dense_mask * scaling * noise_field * (1.0 - identity)
    return (coupled + identity * onsite[None, :]).astype(jnp.bfloat16)


def setup_inputs(seed: int = 0) -> dict:
    streams_of = jax.random.split(jax.random.key(seed), 6)
    hamiltonian = draw_hamiltonian(jax.random.fold_in(streams_of[5], 71), 0)
    tile_pattern = draw_tile_pattern(jax.random.fold_in(streams_of[5], 71), 0)
    n_occ = jax.random.randint(streams_of[2], (1,), NORB // 5, 4 * NORB // 5).astype(jnp.int32)
    mu = jnp.clip(jax.random.uniform(streams_of[3], (1,), jnp.float32, -0.2, 0.2), -0.2, 0.2)
    gamma = jnp.clip(jax.random.uniform(streams_of[4], (1,), jnp.float32, 0.25, 0.4), 0.25, 0.4)
    return dict(hamiltonian=hamiltonian, tile_pattern=tile_pattern, n_occ=n_occ, mu=mu, gamma=gamma)


def reference(hamiltonian, tile_pattern, n_occ, mu, gamma):
    mask = jnp.repeat(jnp.repeat(tile_pattern, TILE, 0), TILE, 1).astype(jnp.float32)
    identity = jnp.eye(NORB, dtype=jnp.float32)
    filling = n_occ[0].astype(jnp.float32) / NORB
    start = mask * (filling * identity + gamma[0] * (mu[0] * identity - hamiltonian.astype(jnp.float32)))
    current = start.astype(jnp.bfloat16)
    result = start
    for iteration in range(STEPS):
        square = mask * jnp.dot(current, current, preferred_element_type=jnp.float32)
        cube = mask * jnp.dot(square.astype(jnp.bfloat16), current, preferred_element_type=jnp.float32)
        result = 3.0 * square - 2.0 * cube
        current = result.astype(jnp.bfloat16)
    return result
```

```python
import functools

import jax
import jax.numpy as jnp
from jax import lax
from jax.experimental import pallas as pl
from jax.experimental.pallas import tpu as pltpu
from jax.sharding import PartitionSpec as P

TILE = 128
STEPS = 2
SUB = 16

SHARE = 80
ROWS = 2 * SHARE
NY, NX, NZ = 4, 4, 8
ROW_BLOCK = SHARE * NZ
BAND_TILES = 10
HALF_TILES = BAND_TILES // 2
WIDTH = HALF_TILES * TILE
TILES = 40
ORDER = TILES * TILE
NSUB = SHARE // SUB
ALL_SLOTS = NY * 2 * NSUB * HALF_TILES
Z_ORDER = (0, -1, 1, -2, 2, -3, 3, 4)
SLOTS = 256
UNROLL = 8
CAPACITY = 88
SPLIT = 40
EXTRA = 16
ROUNDS = -(-(ALL_SLOTS - CAPACITY) // EXTRA)
DEPTH = 4 * TILE

SMEM = pl.BlockSpec(memory_space=pltpu.SMEM)
VMEM = pl.BlockSpec(memory_space=pltpu.VMEM)
ANY = pl.BlockSpec(memory_space=pl.ANY)
PARAMS = pltpu.CompilerParams(vmem_limit_bytes=24 * 1024 * 1024)


def row_of(y, half, z, sub):
    return (2 * y + half) * ROW_BLOCK + SHARE * z + SUB * sub


def col_tile(x, core, t):
    return BAND_TILES * x + 2 * t + core


def where_am_i(pos):
    return pos[0], pos[1], pos[2], pos[3]


def start_kernel(pos, pat, n_occ, mu, gamma, keep, recv, out):
    y, core, x, z = where_am_i(pos)
    filling = jnp.full((SUB, TILE), n_occ[0].astype(jnp.float32)) / ORDER
    apart = lax.broadcasted_iota(jnp.int32, (SUB, TILE), 1) - lax.broadcasted_iota(
        jnp.int32, (SUB, TILE), 0
    )
    for side, ref in ((0, keep), (1, recv)):
        half = core if side == 0 else 1 - core

        def strip(s, _):
            g = row_of(y, half, z, s)
            i = g // TILE
            near = apart == g % TILE
            frm = pl.multiple_of(s * SUB, SUB)
            to = pl.multiple_of(half * SHARE + s * SUB, SUB)
            for t in range(HALF_TILES):
                j = col_tile(x, core, t)
                cols = slice(t * TILE, (t + 1) * TILE)
                identity = jnp.where(near, (i == j).astype(jnp.float32), 0.0)
                h = ref[pl.ds(frm, SUB), cols].astype(jnp.float32)
                value = filling * identity + gamma[0] * (mu[0] * identity - h)
                value = value * pat[i, j].astype(jnp.float32)
                out[pl.ds(to, SUB), cols] = value.astype(jnp.bfloat16)
            return 0

        lax.fori_loop(0, NSUB, strip, 0)


def table_kernel(pos, pat, table, most):
    y, core, x, z = where_am_i(pos)
    f32 = jnp.float32
    full = lax.Precision.HIGHEST
    pattern = pat[...].astype(f32)
    n = NY * 2 * NSUB

    def iota(shape, dim):
        return lax.broadcasted_iota(jnp.int32, shape, dim)

    rows = iota((NZ * n, TILES), 0)
    rz, rn = rows // n, rows % n
    rk = (row_of(rn // (2 * NSUB), rn // NSUB % 2, rz, rn % NSUB)) // TILE
    picked = jnp.dot((rk == iota((NZ * n, TILES), 1)).astype(f32), pattern, precision=full)
    total = jnp.dot(
        (iota((NZ, NZ * n), 0) == iota((NZ, NZ * n), 1) // n).astype(f32), picked, precision=full
    )
    k, group = iota((TILES, 2 * NX), 0), iota((TILES, 2 * NX), 1)
    group = ((k // BAND_TILES) * 2 + k % 2 == group).astype(f32)
    most[0] = jnp.max(jnp.dot(total, group, precision=full)).astype(jnp.int32)

    cols = (iota((TILES, TILE), 0) == col_tile(x, core, iota((TILES, TILE), 1))) & (
        iota((TILES, TILE), 1) < HALF_TILES
    )
    mine = jnp.dot(pattern, cols.astype(f32), precision=full)
    before = (iota((TILE, TILE), 0) < iota((TILE, TILE), 1)).astype(f32)
    below = (iota((n, n), 1) < iota((n, n), 0)).astype(f32)
    slots = iota((n, SLOTS), 1)
    for m, rel in enumerate(Z_ORDER):
        zz = (z + rel) % NZ

        def first_row(shape, dim):
            r = iota(shape, dim)
            return row_of((y + r // (2 * NSUB)) % NY, r // NSUB % 2, zz, r % NSUB)

        pick = (first_row((n, TILES), 0) // TILE == iota((n, TILES), 1)).astype(f32)
        p = jnp.dot(pick, mine, precision=full)
        count = jnp.sum(p, axis=1, keepdims=True)
        ahead = jnp.sum(below * jnp.reshape(jnp.dot(pick, mine, precision=full).sum(axis=1), (1, n)), axis=1, keepdims=True)
        slot = (ahead + jnp.dot(p, before, precision=full)).astype(jnp.int32)
        g = first_row((n, 1), 0)
        kk = g // TILE
        kx, kt = kk // BAND_TILES, kk % BAND_TILES
        place = ((kt + core) % 2 * NX + (kx + NX - x) % NX) * HALF_TILES + kt // 2
        to = (place * TILE + g % TILE) * 8
        r = iota((n, 1), 0)
        frm = (r // NSUB * SHARE + r % NSUB * SUB) * 8
        codes = jnp.zeros((n, SLOTS), jnp.int32)
        sources = jnp.zeros((n, SLOTS), jnp.int32)
        for t in range(HALF_TILES):
            here = (slots == slot[:, t : t + 1]) & (p[:, t : t + 1] > 0)
            codes += jnp.where(here, to + t, 0)
            if m == 0:
                sources += jnp.where(here, frm + t, 0)
        number = jnp.sum(count).astype(jnp.int32)
        at = iota((1, SLOTS), 1)
        line = jnp.sum(codes, axis=0, keepdims=True)
        line = jnp.where(at < number, line, ORDER * 8)
        table[m : m + 1, :] = jnp.where(at == SLOTS - 1, number, line)
        if m == 0:
            table[NZ : NZ + 1, :] = jnp.sum(sources, axis=0, keepdims=True)


def pack_kernel(count, base, table, own, one, two, three, out, block):
    for d, ref in enumerate((own, one, two, three)):
        block[d * ROWS : (d + 1) * ROWS, :] = ref[...]

    def some(i, _):
        for u in range(UNROLL):
            slot = i * UNROLL + u
            code = table[NZ, base[0] + slot]
            row = pl.multiple_of(code // 8, SUB)
            col = pl.multiple_of(code % 8 * TILE, TILE)
            to = pl.multiple_of(slot * SUB, SUB)
            out[pl.ds(to, SUB), :] = block[pl.ds(row, SUB), pl.ds(col, TILE)]
        return 0

    lax.fori_loop(0, count // UNROLL, some, 0)


def place(table, m, source, panel, first, last):
    def some(i, _):
        for u in range(UNROLL):
            slot = first + i * UNROLL + u
            code = table[m, slot]
            row = pl.multiple_of(code // 8, SUB)
            col = pl.multiple_of(code % 8 * TILE, TILE)
            frm = pl.multiple_of((i * UNROLL + u) * SUB, SUB)
            panel[pl.ds(row, SUB), pl.ds(col, TILE)] = source[pl.ds(frm, SUB), :]
        return 0

    number = jnp.clip(table[m, SLOTS - 1] - first, 0, last - first)
    lax.fori_loop(0, (number + UNROLL - 1) // UNROLL, some, 0)


def product(left, panel, rows, total):
    for m, ref in enumerate(left):
        for t in range(HALF_TILES):
            at = (m * HALF_TILES + t) * TILE
            rows[at // DEPTH, :, at % DEPTH : at % DEPTH + TILE] = ref[:, t * TILE : (t + 1) * TILE]
    total[...] = jnp.zeros_like(total)

    def some(m, _):
        at = pl.multiple_of(m * DEPTH, DEPTH)
        total[...] += jnp.dot(
            rows[m], panel[pl.ds(at, DEPTH), :], preferred_element_type=jnp.float32
        )
        return 0

    lax.fori_loop(0, ORDER // DEPTH, some, 0)


def each_tile(pos, pat, use):
    y, core, x, z = where_am_i(pos)

    def strip(q, _):
        i = row_of(y, q // NSUB, z, q % NSUB) // TILE
        at = pl.multiple_of(q // NSUB * SHARE + q % NSUB * SUB, SUB)
        for t in range(HALF_TILES):
            where = (pl.ds(at, SUB), slice(t * TILE, (t + 1) * TILE))
            use(where, pat[i, col_tile(x, core, t)].astype(jnp.float32))
        return 0

    lax.fori_loop(0, 2 * NSUB, strip, 0)


def square_kernel(pos, pat, table, *refs):
    packed, left, spill = refs[:9], refs[9:17], refs[17]
    (square, square_half, panel), (rows, total, more) = refs[18:21], refs[21:]
    panel[...] = jnp.zeros_like(panel)
    for m in range(NZ - 1):
        place(table, m, packed[m], panel, 0, CAPACITY)
    place(table, NZ - 1, packed[NZ - 1], panel, 0, SPLIT)
    place(table, NZ - 1, packed[NZ], panel, SPLIT, CAPACITY)
    for m in range(NZ):

        @pl.when(table[m, SLOTS - 1] > CAPACITY)
        def _():
            pltpu.sync_copy(spill.at[m], more)
            place(table, m, more, panel, CAPACITY, CAPACITY + ROUNDS * EXTRA)

    product(left, panel, rows, total)

    def use(where, mask):
        value = total[where] * mask
        square[where] = value
        square_half[where] = value.astype(jnp.bfloat16)

    each_tile(pos, pat, use)


def cube_kernel(pos, pat, square, panel, *refs):
    left, out, (rows, total) = refs[:8], refs[8], refs[9:]
    product(left, panel, rows, total)

    def use(where, mask):
        value = 3.0 * square[where] - 2.0 * (total[where] * mask)
        out[where] = value.astype(out.dtype)

    each_tile(pos, pat, use)


def ring(axis, shift, size, stride=1):
    return [(i, (i + shift * stride) % size) for i in range(size)]


def along_x(value, shift):
    return lax.ppermute(value, "col", ring("col", shift, NX))


def along_y(value, shift):
    return lax.ppermute(value, "row", ring("row", shift, 2 * NY, 2))


def along_z(value, shift):
    return lax.ppermute(value, "layer", ring("layer", shift, NZ))


def other_core(value):
    return lax.ppermute(value, "row", [(i, i ^ 1) for i in range(2 * NY)])


def whole_rows(half_rows):
    pieces = [half_rows, along_x(half_rows, -1), along_x(half_rows, 2), along_x(half_rows, 1)]
    return pieces + [other_core(piece) for piece in pieces]


def call(kernel, outs, n_smem, *args, scratch=(), n_any=0, flops=0):
    single = not isinstance(outs, (tuple, list))
    return pl.pallas_call(
        kernel,
        out_shape=outs,
        in_specs=[SMEM] * n_smem + [VMEM] * (len(args) - n_smem - n_any) + [ANY] * n_any,
        out_specs=VMEM if single else [VMEM] * len(outs),
        scratch_shapes=scratch,
        compiler_params=PARAMS,
        cost_estimate=pl.CostEstimate(flops=flops, bytes_accessed=0, transcendentals=0),
    )(*args)


def pack(count, base, table, blocks):
    return call(
        functools.partial(pack_kernel, count),
        jax.ShapeDtypeStruct((count * SUB, TILE), jnp.bfloat16),
        2,
        *(jnp.asarray(base, jnp.int32).reshape(1), table, *blocks),
        scratch=(pltpu.VMEM((NY * ROWS, WIDTH), jnp.bfloat16),),
    )


def nothing_kernel(out):
    pass


def spilled(most, table, blocks):
    rounds = (most[0] - CAPACITY + EXTRA - 1) // EXTRA
    shape = (NZ, ROUNDS * EXTRA * SUB, TILE)
    empty = pl.pallas_call(
        nothing_kernel, out_shape=jax.ShapeDtypeStruct(shape, jnp.bfloat16), out_specs=ANY
    )()

    def one_round(carry):
        turn, spill = carry
        mine = pack(EXTRA, CAPACITY + turn * EXTRA, table, blocks)
        got = [mine] + [along_z(mine, -rel) for rel in Z_ORDER[1:]]
        at = (0, turn * EXTRA * SUB, 0)
        return turn + 1, lax.dynamic_update_slice(spill, jnp.stack(got), at)

    return lax.while_loop(lambda carry: carry[0] < rounds, one_round, (jnp.int32(0), empty))[1]


def steps(pos, pat, current, table, most):
    f32 = jax.ShapeDtypeStruct((ROWS, WIDTH), jnp.float32)
    bf16 = jax.ShapeDtypeStruct((ROWS, WIDTH), jnp.bfloat16)
    panel_shape = jax.ShapeDtypeStruct((ORDER + SUB, WIDTH), jnp.bfloat16)
    work = (
        pltpu.VMEM((ORDER // DEPTH, ROWS, DEPTH), jnp.bfloat16),
        pltpu.VMEM((ROWS, WIDTH), jnp.float32),
    )
    more = (pltpu.VMEM((ROUNDS * EXTRA * SUB, TILE), jnp.bfloat16),)
    split = SPLIT * SUB
    for step in range(STEPS):
        blocks = (current, along_y(current, -1), along_y(current, 2), along_y(current, 1))
        packed = pack(CAPACITY, 0, table, blocks)
        down, up = along_z(packed, 1), along_z(packed, -1)
        down2, up2 = along_z(packed, 2), along_z(packed, -2)
        current, _ = lax.optimization_barrier((current, packed))
        left = whole_rows(current)
        down3, up3 = along_z(down2, 1), along_z(up2, -1)
        far_a, far_b = along_z(down2[:split], 2), along_z(up2[split:], -2)
        spill = spilled(most, table, blocks)
        square, square_half, panel = call(
            square_kernel,
            (f32, bf16, panel_shape),
            3,
            *(pos, pat, table, packed, down, up, down2, up2, down3, up3, far_a, far_b),
            *left,
            spill,
            scratch=work + more,
            n_any=1,
            flops=10**9,
        )
        left = whole_rows(square_half)
        out = f32 if step == STEPS - 1 else bf16
        current = call(cube_kernel, out, 2, pos, pat, square, panel, *left, scratch=work, flops=10**9)
    return current


def shards(hamiltonian, tile_pattern, n_occ, mu, gamma):
    row, x, z = lax.axis_index("row"), lax.axis_index("col"), lax.axis_index("layer")
    y, core = row // 2, row % 2
    pos = jnp.stack([y, core, x, z]).astype(jnp.int32)
    tiles = hamiltonian.reshape(SHARE, HALF_TILES, 2, TILE)
    even, odd = tiles[:, :, 0].reshape(SHARE, WIDTH), tiles[:, :, 1].reshape(SHARE, WIDTH)
    first = core == 0
    keep, send = jnp.where(first, even, odd), jnp.where(first, odd, even)
    recv = other_core(send)
    bf16 = jax.ShapeDtypeStruct((ROWS, WIDTH), jnp.bfloat16)
    current = call(start_kernel, bf16, 5, pos, tile_pattern, n_occ, mu, gamma, keep, recv)
    table, most = pl.pallas_call(
        table_kernel,
        out_shape=(
            jax.ShapeDtypeStruct((NZ + 1, SLOTS), jnp.int32),
            jax.ShapeDtypeStruct((1,), jnp.int32),
        ),
        in_specs=[SMEM, VMEM],
        out_specs=[VMEM, SMEM],
        compiler_params=PARAMS,
    )(pos, tile_pattern)
    result = steps(pos, tile_pattern, current, table, most)
    mine = jnp.where(first, result[:SHARE], result[SHARE:])
    theirs = other_core(jnp.where(first, result[SHARE:], result[:SHARE]))
    even, odd = jnp.where(first, mine, theirs), jnp.where(first, theirs, mine)
    both = jnp.stack([even.reshape(SHARE, HALF_TILES, TILE), odd.reshape(SHARE, HALF_TILES, TILE)], axis=2)
    return both.reshape(SHARE, 2 * WIDTH)


def solution(mesh):
    placed = (P(("row", "layer"), "col"), P(), P(), P(), P())
    return jax.shard_map(
        shards, mesh=mesh, in_specs=placed, out_specs=P(("row", "layer"), "col"), check_vma=False
    )
```

```python
import functools
import math

import jax
import jax.numpy as jnp
from jax import lax
from jax.experimental import pallas as pl
from jax.experimental.pallas import tpu as pltpu
from jax.sharding import PartitionSpec as P

TILE = 128
STEPS = 2
SUB = 16

SHARE = 80
ROWS = 2 * SHARE
NY, NX, NZ = 4, 4, 8
ROW_BLOCK = SHARE * NZ
BAND_TILES = 10
HALF_TILES = BAND_TILES // 2
WIDTH = HALF_TILES * TILE
TILES = 40
ORDER = TILES * TILE
NSUB = SHARE // SUB
ALL_SLOTS = NY * 2 * NSUB * HALF_TILES
Z_ORDER = (0, -1, 1, -2, 2, -3, 3, 4)
SLOTS = 256
UNROLL = 8
CAPACITY = 96
SPLIT = 48
EXTRA = 16
ROUNDS = -(-(ALL_SLOTS - CAPACITY) // EXTRA)
DEPTH = 4 * TILE

SMEM = pl.BlockSpec(memory_space=pltpu.SMEM)
VMEM = pl.BlockSpec(memory_space=pltpu.VMEM)
ANY = pl.BlockSpec(memory_space=pl.ANY)
PARAMS = pltpu.CompilerParams(vmem_limit_bytes=14 * 1024 * 1024)


def row_of(y, half, z, sub):
    return (2 * y + half) * ROW_BLOCK + SHARE * z + SUB * sub


def col_tile(x, core, t):
    return BAND_TILES * x + 2 * t + core


def where_am_i(pos):
    return pos[0], pos[1], pos[2], pos[3]


def split_kernel(pos, whole, keep, send):
    y, core, x, z = where_am_i(pos)
    for t in range(HALF_TILES):
        at = slice(t * TILE, (t + 1) * TILE)
        mine = pl.multiple_of((2 * t + core) * TILE, TILE)
        other = pl.multiple_of((2 * t + 1 - core) * TILE, TILE)
        keep[:, at] = whole[:, pl.ds(mine, TILE)]
        send[:, at] = whole[:, pl.ds(other, TILE)]


def merge_kernel(pos, result, theirs, whole):
    y, core, x, z = where_am_i(pos)
    rows = pl.ds(pl.multiple_of(core * SHARE, SHARE), SHARE)
    for t in range(HALF_TILES):
        at = slice(t * TILE, (t + 1) * TILE)
        mine = pl.multiple_of((2 * t + core) * TILE, TILE)
        other = pl.multiple_of((2 * t + 1 - core) * TILE, TILE)
        whole[:, pl.ds(mine, TILE)] = result[rows, at]
        whole[:, pl.ds(other, TILE)] = theirs[:, at]


def start_kernel(pos, pat, n_occ, mu, gamma, keep, recv, out):
    y, core, x, z = where_am_i(pos)
    filling = jnp.full((SUB, TILE), n_occ[0].astype(jnp.float32)) / ORDER
    apart = lax.broadcasted_iota(jnp.int32, (SUB, TILE), 1) - lax.broadcasted_iota(
        jnp.int32, (SUB, TILE), 0
    )
    for side, ref in ((0, keep), (1, recv)):
        half = core if side == 0 else 1 - core

        def strip(s, _):
            g = row_of(y, half, z, s)
            i = g // TILE
            near = apart == g % TILE
            frm = pl.multiple_of(s * SUB, SUB)
            to = pl.multiple_of(half * SHARE + s * SUB, SUB)
            for t in range(HALF_TILES):
                j = col_tile(x, core, t)
                cols = slice(t * TILE, (t + 1) * TILE)
                identity = jnp.where(near, (i == j).astype(jnp.float32), 0.0)
                h = ref[pl.ds(frm, SUB), cols].astype(jnp.float32)
                value = filling * identity + gamma[0] * (mu[0] * identity - h)
                value = value * pat[i, j].astype(jnp.float32)
                out[pl.ds(to, SUB), cols] = value.astype(jnp.bfloat16)
            return 0

        lax.fori_loop(0, NSUB, strip, 0)


def table_kernel(pos, pat, table, most):
    y, core, x, z = where_am_i(pos)
    f32 = jnp.float32
    pattern = pat[...].astype(f32)
    n = NY * 2 * NSUB

    def iota(shape, dim):
        return lax.broadcasted_iota(jnp.int32, shape, dim)

    rows = iota((NZ * n, TILES), 0)
    rz, rn = rows // n, rows % n
    rk = (row_of(rn // (2 * NSUB), rn // NSUB % 2, rz, rn % NSUB)) // TILE
    picked = jnp.dot((rk == iota((NZ * n, TILES), 1)).astype(f32), pattern)
    total = jnp.dot(
        (iota((NZ, NZ * n), 0) == iota((NZ, NZ * n), 1) // n).astype(f32), picked
    )
    k, group = iota((TILES, 2 * NX), 0), iota((TILES, 2 * NX), 1)
    group = ((k // BAND_TILES) * 2 + k % 2 == group).astype(f32)
    most[0] = jnp.max(jnp.dot(total, group)).astype(jnp.int32)

    cols = (iota((TILES, TILE), 0) == col_tile(x, core, iota((TILES, TILE), 1))) & (
        iota((TILES, TILE), 1) < HALF_TILES
    )
    mine = jnp.dot(pattern, cols.astype(f32))
    before = (iota((TILE, TILE), 0) < iota((TILE, TILE), 1)).astype(f32)
    below = (iota((n, n), 1) < iota((n, n), 0)).astype(f32)
    slots = iota((n, SLOTS), 1)
    for m, rel in enumerate(Z_ORDER):
        zz = (z + rel) % NZ

        def first_row(shape, dim):
            r = iota(shape, dim)
            return row_of((y + r // (2 * NSUB)) % NY, r // NSUB % 2, zz, r % NSUB)

        pick = (first_row((n, TILES), 0) // TILE == iota((n, TILES), 1)).astype(f32)
        p = jnp.dot(pick, mine)
        count = jnp.sum(p, axis=1, keepdims=True)
        ahead = jnp.sum(below * jnp.reshape(jnp.dot(pick, mine).sum(axis=1), (1, n)), axis=1, keepdims=True)
        slot = (ahead + jnp.dot(p, before)).astype(jnp.int32)
        g = first_row((n, 1), 0)
        kk = g // TILE
        kx, kt = kk // BAND_TILES, kk % BAND_TILES
        place = ((kt + core) % 2 * NX + (kx + NX - x) % NX) * HALF_TILES + kt // 2
        to = (place * TILE + g % TILE) * 8
        r = iota((n, 1), 0)
        frm = (r // NSUB * SHARE + r % NSUB * SUB) * 8
        codes = jnp.zeros((n, SLOTS), jnp.int32)
        sources = jnp.zeros((n, SLOTS), jnp.int32)
        for t in range(HALF_TILES):
            here = (slots == slot[:, t : t + 1]) & (p[:, t : t + 1] > 0)
            codes += jnp.where(here, to + t, 0)
            if m == 0:
                sources += jnp.where(here, frm + t, 0)
        number = jnp.sum(count).astype(jnp.int32)
        at = iota((1, SLOTS), 1)
        line = jnp.sum(codes, axis=0, keepdims=True)
        line = jnp.where(at < number, line, ORDER * 8)
        table[m : m + 1, :] = jnp.where(at == SLOTS - 1, number, line)
        if m == 0:
            table[NZ : NZ + 1, :] = jnp.sum(sources, axis=0, keepdims=True)


def pack_kernel(count, base, table, own, one, two, three, out, block):
    for d, ref in enumerate((own, one, two, three)):
        block[d * ROWS : (d + 1) * ROWS, :] = ref[...]

    def some(i, _):
        for u in range(UNROLL):
            slot = i * UNROLL + u
            code = table[NZ, base[0] + slot]
            row = pl.multiple_of(code // 8, SUB)
            col = pl.multiple_of(code % 8 * TILE, TILE)
            to = pl.multiple_of(slot * SUB, SUB)
            out[pl.ds(to, SUB), :] = block[pl.ds(row, SUB), pl.ds(col, TILE)]
        return 0

    lax.fori_loop(0, count // UNROLL, some, 0)


def place(table, m, source, panel, first, last):
    def some(i, _):
        for u in range(UNROLL):
            slot = first + i * UNROLL + u
            code = table[m, slot]
            row = pl.multiple_of(code // 8, SUB)
            col = pl.multiple_of(code % 8 * TILE, TILE)
            frm = pl.multiple_of((i * UNROLL + u) * SUB, SUB)
            panel[pl.ds(row, SUB), pl.ds(col, TILE)] = source[pl.ds(frm, SUB), :]
        return 0

    number = jnp.clip(table[m, SLOTS - 1] - first, 0, last - first)
    lax.fori_loop(0, (number + UNROLL - 1) // UNROLL, some, 0)


def product(left, panel, rows, total):
    for m, ref in enumerate(left):
        for t in range(HALF_TILES):
            at = (m * HALF_TILES + t) * TILE
            rows[at // DEPTH, :, at % DEPTH : at % DEPTH + TILE] = ref[:, t * TILE : (t + 1) * TILE]
    total[...] = jnp.zeros_like(total)

    def some(m, _):
        at = pl.multiple_of(m * DEPTH, DEPTH)
        total[...] += jnp.dot(
            rows[m], panel[pl.ds(at, DEPTH), :], preferred_element_type=jnp.float32
        )
        return 0

    lax.fori_loop(0, ORDER // DEPTH, some, 0)


def each_tile(pos, pat, use):
    y, core, x, z = where_am_i(pos)

    def strip(q, _):
        i = row_of(y, q // NSUB, z, q % NSUB) // TILE
        at = pl.multiple_of(q // NSUB * SHARE + q % NSUB * SUB, SUB)
        for t in range(HALF_TILES):
            where = (pl.ds(at, SUB), slice(t * TILE, (t + 1) * TILE))
            use(where, pat[i, col_tile(x, core, t)].astype(jnp.float32))
        return 0

    lax.fori_loop(0, 2 * NSUB, strip, 0)


def square_kernel(pos, pat, table, *refs):
    packed, left, spill = refs[:9], refs[9:17], refs[17]
    (square, square_half, panel), (rows, total, more) = refs[18:21], refs[21:]
    panel[...] = jnp.zeros_like(panel)
    for m in range(NZ - 1):
        place(table, m, packed[m], panel, 0, CAPACITY)
    place(table, NZ - 1, packed[NZ - 1], panel, 0, SPLIT)
    place(table, NZ - 1, packed[NZ], panel, SPLIT, CAPACITY)
    for m in range(NZ):

        @pl.when(table[m, SLOTS - 1] > CAPACITY)
        def _():
            pltpu.sync_copy(spill.at[m], more)
            place(table, m, more, panel, CAPACITY, CAPACITY + ROUNDS * EXTRA)

    product(left, panel, rows, total)

    def use(where, mask):
        value = total[where] * mask
        square[where] = value
        square_half[where] = value.astype(jnp.bfloat16)

    each_tile(pos, pat, use)


def cube_kernel(pos, pat, square, panel, *refs):
    left, (out, out_half), (rows, total) = refs[:8], refs[8:10], refs[10:]
    product(left, panel, rows, total)

    def use(where, mask):
        value = 3.0 * square[where] - 2.0 * (total[where] * mask)
        out[where] = value
        out_half[where] = value.astype(jnp.bfloat16)

    each_tile(pos, pat, use)


def ring(axis, shift, size, stride=1):
    return [(i, (i + shift * stride) % size) for i in range(size)]


def along_x(value, shift):
    return lax.ppermute(value, "col", ring("col", shift, NX))


def along_y(value, shift):
    return lax.ppermute(value, "row", ring("row", shift, 2 * NY, 2))


def along_z(value, shift):
    return lax.ppermute(value, "layer", ring("layer", shift, NZ))


def other_core(value):
    return lax.ppermute(value, "row", [(i, i ^ 1) for i in range(2 * NY)])


def whole_rows(half_rows):
    pieces = [half_rows, along_x(half_rows, -1), along_x(half_rows, 2), along_x(half_rows, 1)]
    return pieces + [other_core(piece) for piece in pieces]


def call(kernel, outs, n_smem, *args, scratch=(), n_any=0, flops=0):
    single = not isinstance(outs, (tuple, list))
    arrays = [*args, outs] if single else [*args, *outs]
    touched = sum(math.prod(a.shape) * jnp.dtype(a.dtype).itemsize for a in arrays)
    return pl.pallas_call(
        kernel,
        out_shape=outs,
        in_specs=[SMEM] * n_smem + [VMEM] * (len(args) - n_smem - n_any) + [ANY] * n_any,
        out_specs=VMEM if single else [VMEM] * len(outs),
        scratch_shapes=scratch,
        compiler_params=PARAMS,
        cost_estimate=pl.CostEstimate(flops=flops, bytes_accessed=touched, transcendentals=0),
    )(*args)


def pack(count, base, table, blocks):
    return call(
        functools.partial(pack_kernel, count),
        jax.ShapeDtypeStruct((count * SUB, TILE), jnp.bfloat16),
        2,
        *(jnp.asarray(base, jnp.int32).reshape(1), table, *blocks),
        scratch=(pltpu.VMEM((NY * ROWS, WIDTH), jnp.bfloat16),),
    )


def nothing_kernel(out):
    pass


def spilled(most, table, blocks):
    rounds = (most[0] - CAPACITY + EXTRA - 1) // EXTRA
    shape = (NZ, ROUNDS * EXTRA * SUB, TILE)
    empty = pl.pallas_call(
        nothing_kernel, out_shape=jax.ShapeDtypeStruct(shape, jnp.bfloat16), out_specs=ANY
    )()

    def one_round(carry):
        turn, spill = carry
        mine = pack(EXTRA, CAPACITY + turn * EXTRA, table, blocks)
        got = [mine] + [along_z(mine, -rel) for rel in Z_ORDER[1:]]
        at = (0, turn * EXTRA * SUB, 0)
        return turn + 1, lax.dynamic_update_slice(spill, jnp.stack(got), at)

    return lax.while_loop(lambda carry: carry[0] < rounds, one_round, (jnp.int32(0), empty))[1]


def steps(pos, pat, current, table, most):
    f32 = jax.ShapeDtypeStruct((ROWS, WIDTH), jnp.float32)
    bf16 = jax.ShapeDtypeStruct((ROWS, WIDTH), jnp.bfloat16)
    panel_shape = jax.ShapeDtypeStruct((ORDER + SUB, WIDTH), jnp.bfloat16)
    work = (
        pltpu.VMEM((ORDER // DEPTH, ROWS, DEPTH), jnp.bfloat16),
        pltpu.VMEM((ROWS, WIDTH), jnp.float32),
    )
    more = (pltpu.VMEM((ROUNDS * EXTRA * SUB, TILE), jnp.bfloat16),)
    split = SPLIT * SUB

    def step(carry):
        turn, current = carry[:2]
        blocks = (current, along_y(current, -1), along_y(current, 2), along_y(current, 1))
        packed = pack(CAPACITY, 0, table, blocks)
        turn, current, packed = lax.optimization_barrier((turn + 1, current, packed))
        down, up = along_z(packed, 1), along_z(packed, -1)
        down2, up2 = along_z(down, 1), along_z(up, -1)
        down3, up3 = along_z(down2, 1), along_z(up2, -1)
        far_a, far_b = along_z(down3[:split], 1), along_z(up3[split:], -1)
        left = whole_rows(current)
        spill = spilled(most, table, blocks)
        square, square_half, panel = call(
            square_kernel,
            (f32, bf16, panel_shape),
            3,
            *(pos, pat, table, packed, down, up, down2, up2, down3, up3, far_a, far_b),
            *left,
            spill,
            scratch=work + more,
            n_any=1,
            flops=10**9,
        )
        left = whole_rows(square_half)
        result, following = call(
            cube_kernel, (f32, bf16), 2, pos, pat, square, panel, *left, scratch=work, flops=10**9
        )
        return turn, following, result

    first = (jnp.int32(0), current, jnp.zeros((ROWS, WIDTH), jnp.float32))
    return lax.while_loop(lambda carry: carry[0] < STEPS, step, first)[2]


def shards(hamiltonian, tile_pattern, n_occ, mu, gamma):
    row, x, z = lax.axis_index("row"), lax.axis_index("col"), lax.axis_index("layer")
    y, core = row // 2, row % 2
    pos = jnp.stack([y, core, x, z]).astype(jnp.int32)
    share = jax.ShapeDtypeStruct((SHARE, WIDTH), jnp.bfloat16)
    keep, send = call(split_kernel, (share, share), 1, pos, hamiltonian)
    recv = other_core(send)
    bf16 = jax.ShapeDtypeStruct((ROWS, WIDTH), jnp.bfloat16)
    current = call(start_kernel, bf16, 5, pos, tile_pattern, n_occ, mu, gamma, keep, recv)
    table, most = pl.pallas_call(
        table_kernel,
        out_shape=(
            jax.ShapeDtypeStruct((NZ + 1, SLOTS), jnp.int32),
            jax.ShapeDtypeStruct((1,), jnp.int32),
        ),
        in_specs=[SMEM, VMEM],
        out_specs=[VMEM, SMEM],
        compiler_params=PARAMS,
    )(pos, tile_pattern)
    result = steps(pos, tile_pattern, current, table, most)
    theirs = other_core(jnp.where(core == 0, result[SHARE:], result[:SHARE]))
    whole = jax.ShapeDtypeStruct((SHARE, 2 * WIDTH), jnp.float32)
    return call(merge_kernel, whole, 1, pos, result, theirs)


def solution(mesh):
    placed = (P(("row", "layer"), "col"), P(), P(), P(), P())
    return jax.shard_map(
        shards, mesh=mesh, in_specs=placed, out_specs=P(("row", "layer"), "col"), check_vma=False
    )
```

```python
import functools

import jax
import jax.numpy as jnp
from jax import lax
from jax.experimental import pallas as pl
from jax.experimental.pallas import tpu as pltpu
from jax.sharding import PartitionSpec as P

TILE = 128
STEPS = 2
SUB = 16

SHARE = 80
NY, NX, NZ = 4, 4, 8
ROW_BLOCK = SHARE * NZ
BAND_TILES = 10
WIDTH = BAND_TILES * TILE
TILES = 40
ORDER = TILES * TILE
NSUB = SHARE // SUB
ALL_SLOTS = 2 * NY * NSUB * BAND_TILES
Z_ORDER = (0, -1, 1, -2, 2, -3, 3, 4)
SLOTS = 512
UNROLL = 8
CAPACITY = 88
SPLIT = 48
EXTRA = 16
ROUNDS = -(-(ALL_SLOTS // 2 - CAPACITY) // EXTRA)

SMEM = pl.BlockSpec(memory_space=pltpu.SMEM)
VMEM = pl.BlockSpec(memory_space=pltpu.VMEM)
HBM = pl.BlockSpec(memory_space=pltpu.HBM)
PARAMS = pltpu.CompilerParams(vmem_limit_bytes=20 * 1024 * 1024)


def row_of(block, z, sub):
    return block * ROW_BLOCK + SHARE * z + SUB * sub


def where_am_i(pos):
    return pos[0], pos[1], pos[2], pos[3]


def start_kernel(pos, pat, n_occ, mu, gamma, hamiltonian, out):
    y, core, x, z = where_am_i(pos)
    filling = jnp.full((SUB, TILE), n_occ[0].astype(jnp.float32)) / ORDER
    apart = lax.broadcasted_iota(jnp.int32, (SUB, TILE), 1) - lax.broadcasted_iota(
        jnp.int32, (SUB, TILE), 0
    )

    def strip(s, _):
        g = row_of(2 * y + core, z, s)
        i = g // TILE
        near = apart == g % TILE
        rows = pl.ds(pl.multiple_of(s * SUB, SUB), SUB)
        for t in range(BAND_TILES):
            j = BAND_TILES * x + t
            cols = slice(t * TILE, (t + 1) * TILE)
            identity = jnp.where(near, (i == j).astype(jnp.float32), 0.0)
            h = hamiltonian[rows, cols].astype(jnp.float32)
            value = filling * identity + gamma[0] * (mu[0] * identity - h)
            out[rows, cols] = (value * pat[i, j].astype(jnp.float32)).astype(jnp.bfloat16)
        return 0

    lax.fori_loop(0, NSUB, strip, 0)


def table_kernel(pos, pat, table, most):
    y, core, x, z = where_am_i(pos)
    f32 = jnp.float32
    pattern = pat[...].astype(f32)
    n = 8 * NSUB

    def iota(shape, dim):
        return lax.broadcasted_iota(jnp.int32, shape, dim)

    rows = iota((NZ * n, TILES), 0)
    rz, rn = rows // n, rows % n
    rk = row_of(rn // NSUB, rz, rn % NSUB) // TILE
    picked = jnp.dot((rk == iota((NZ * n, TILES), 1)).astype(f32), pattern)
    total = jnp.dot(
        (iota((NZ, NZ * n), 0) == iota((NZ, NZ * n), 1) // n).astype(f32), picked
    )
    k, band = iota((TILES, NX), 0), iota((TILES, NX), 1)
    group = (k // BAND_TILES == band).astype(f32)
    most[0] = jnp.max(jnp.dot(total, group)).astype(jnp.int32)

    cols = (iota((TILES, TILE), 0) == BAND_TILES * x + iota((TILES, TILE), 1)) & (
        iota((TILES, TILE), 1) < BAND_TILES
    )
    mine = jnp.dot(pattern, cols.astype(f32))
    before = (iota((TILE, TILE), 0) < iota((TILE, TILE), 1)).astype(f32)
    below = (iota((n, n), 1) < iota((n, n), 0)).astype(f32)
    slots = iota((n, SLOTS), 1)
    for m, rel in enumerate(Z_ORDER):
        zz = (z + rel) % NZ

        def first_row(shape, dim):
            r = iota(shape, dim)
            return row_of((2 * y + r // NSUB) % (2 * NY), zz, r % NSUB)

        pick = (first_row((n, TILES), 0) // TILE == iota((n, TILES), 1)).astype(f32)
        p = jnp.dot(pick, mine)
        count = jnp.sum(p, axis=1, keepdims=True)
        ahead = jnp.sum(below * jnp.reshape(jnp.dot(pick, mine).sum(axis=1), (1, n)), axis=1, keepdims=True)
        slot = (ahead + jnp.dot(p, before)).astype(jnp.int32)
        g = first_row((n, 1), 0)
        kk = g // TILE
        kx, kt = kk // BAND_TILES, kk % BAND_TILES
        place = (kx + NX - x) % NX * BAND_TILES + kt
        to = (place * TILE + g % TILE) * 16
        r = iota((n, 1), 0)
        frm = (r // NSUB * SHARE + r % NSUB * SUB) * 16
        codes = jnp.zeros((n, SLOTS), jnp.int32)
        sources = jnp.zeros((n, SLOTS), jnp.int32)
        for t in range(BAND_TILES):
            here = (slots == slot[:, t : t + 1]) & (p[:, t : t + 1] > 0)
            codes += jnp.where(here, to + t, 0)
            if m == 0:
                sources += jnp.where(here, frm + t, 0)
        number = jnp.sum(count).astype(jnp.int32)
        at = iota((1, SLOTS), 1)
        line = jnp.sum(codes, axis=0, keepdims=True)
        line = jnp.where(at < number, line, ORDER * 16)
        table[m : m + 1, :] = jnp.where(at == SLOTS - 1, number, line)
        if m == 0:
            table[NZ : NZ + 1, :] = jnp.sum(sources, axis=0, keepdims=True)


def pack_kernel(count, pos, base, table, *refs):
    blocks, (out, block) = refs[:8], refs[8:]
    core = pos[1]
    for d, ref in enumerate(blocks):
        at = d % NY * 2 + (core if d < NY else 1 - core)
        block[pl.ds(pl.multiple_of(at * SHARE, SHARE), SHARE), :] = ref[...]

    def some(i, _):
        for u in range(UNROLL):
            slot = i * UNROLL + u
            code = table[NZ, 2 * (base[0] + slot) + core]
            row = pl.multiple_of(code // 16, SUB)
            col = pl.multiple_of(code % 16 * TILE, TILE)
            to = pl.multiple_of(slot * SUB, SUB)
            out[pl.ds(to, SUB), :] = block[pl.ds(row, SUB), pl.ds(col, TILE)]
        return 0

    lax.fori_loop(0, count // UNROLL, some, 0)


def place(table, m, core, source, panel, first, last):
    def some(i, _):
        for u in range(UNROLL):
            slot = first + i * UNROLL + u
            code = table[m, 2 * slot + core]
            row = pl.multiple_of(code // 16, SUB)
            col = pl.multiple_of(code % 16 * TILE, TILE)
            frm = pl.multiple_of((i * UNROLL + u) * SUB, SUB)
            panel[pl.ds(row, SUB), pl.ds(col, TILE)] = source[pl.ds(frm, SUB), :]
        return 0

    number = jnp.clip((table[m, SLOTS - 1] + 1 - core) // 2 - first, 0, last - first)
    lax.fori_loop(0, (number + UNROLL - 1) // UNROLL, some, 0)


def product(left, panel):
    total = None
    for m, ref in enumerate(left):
        at = slice(m * WIDTH, (m + 1) * WIDTH)
        one = jnp.dot(ref[...], panel[at, :], preferred_element_type=jnp.float32)
        total = one if total is None else total + one
    return total


def each_tile(pos, pat, use):
    y, core, x, z = where_am_i(pos)

    def strip(s, _):
        i = row_of(2 * y + core, z, s) // TILE
        rows = pl.ds(pl.multiple_of(s * SUB, SUB), SUB)
        for t in range(BAND_TILES):
            where = (rows, slice(t * TILE, (t + 1) * TILE))
            use(where, pat[i, BAND_TILES * x + t].astype(jnp.float32))
        return 0

    lax.fori_loop(0, NSUB, strip, 0)


def parts_kernel(down, up, first, last):
    first[...] = down[: SPLIT * SUB, :]
    last[...] = up[SPLIT * SUB :, :]


def near_kernel(pos, table, *refs):
    packed, panel = refs[:-1], refs[-1]
    panel[...] = jnp.zeros_like(panel)
    for q, ref in enumerate(packed):
        core = pos[1] if q % 2 == 0 else 1 - pos[1]
        place(table, q // 2, core, ref, panel, 0, CAPACITY)


def square_kernel(pos, pat, table, *refs):
    packed, left, spill = refs[:8], refs[9:13], refs[13]
    (square, square_half, panel), (total, more) = refs[14:17], refs[17:]
    for q, ref in enumerate(packed):
        core = pos[1] if q % 2 == 0 else 1 - pos[1]
        m = (5, 6, 7, 7)[q // 2]
        first, last = ((0, CAPACITY), (0, CAPACITY), (0, SPLIT), (SPLIT, CAPACITY))[q // 2]
        place(table, m, core, ref, panel, first, last)
    for m in range(NZ):

        @pl.when(table[m, SLOTS - 1] > 2 * CAPACITY)
        def _():
            for side in range(2):
                core = pos[1] if side == 0 else 1 - pos[1]
                pltpu.sync_copy(spill.at[side, (pos[3] + Z_ORDER[m] + NZ) % NZ], more)
                place(table, m, core, more, panel, CAPACITY, CAPACITY + ROUNDS * EXTRA)

    total[...] = product(left, panel)

    def use(where, mask):
        value = total[where] * mask
        square[where] = value
        square_half[where] = value.astype(jnp.bfloat16)

    each_tile(pos, pat, use)


def cube_kernel(pos, pat, square, panel, *refs):
    left, (out, out_half), total = refs[:4], refs[4:6], refs[6]
    total[...] = product(left, panel)

    def use(where, mask):
        value = 3.0 * square[where] - 2.0 * (total[where] * mask)
        out[where] = value
        out_half[where] = value.astype(jnp.bfloat16)

    each_tile(pos, pat, use)


def ring(axis, shift, size, stride=1):
    return [(i, (i + shift * stride) % size) for i in range(size)]


def along_x(value, shift):
    return lax.ppermute(value, "col", ring("col", shift, NX))


def along_y(value, shift):
    return lax.ppermute(value, "row", ring("row", shift, 2 * NY, 2))


def along_z(value, shift):
    return lax.ppermute(value, "layer", ring("layer", shift, NZ))


def other_core(value):
    return lax.ppermute(value, "row", [(i, i ^ 1) for i in range(2 * NY)])


def whole_rows(mine):
    return [mine, along_x(mine, -1), along_x(mine, 2), along_x(mine, 1)]


def call(kernel, outs, n_smem, *args, scratch=(), n_hbm=0, flops=0, aliases=None):
    single = not isinstance(outs, (tuple, list))
    return pl.pallas_call(
        kernel,
        out_shape=outs,
        in_specs=[SMEM] * n_smem + [VMEM] * (len(args) - n_smem - n_hbm) + [HBM] * n_hbm,
        out_specs=VMEM if single else [VMEM] * len(outs),
        scratch_shapes=scratch,
        input_output_aliases=aliases or {},
        compiler_params=PARAMS,
        cost_estimate=pl.CostEstimate(flops=flops, bytes_accessed=0, transcendentals=0),
    )(*args)


def pack(count, pos, base, table, blocks):
    return call(
        functools.partial(pack_kernel, count),
        jax.ShapeDtypeStruct((count * SUB, TILE), jnp.bfloat16),
        3,
        *(pos, jnp.asarray(base, jnp.int32).reshape(1), table, *blocks),
        scratch=(pltpu.VMEM((ROW_BLOCK, WIDTH), jnp.bfloat16),),
    )


def nothing_kernel(out):
    pass


def spilled(pos, most, table, blocks):
    rounds = (most[0] - 2 * CAPACITY + 2 * EXTRA - 1) // (2 * EXTRA)
    shape = (2, NZ, ROUNDS * EXTRA * SUB, TILE)
    empty = pl.pallas_call(
        nothing_kernel, out_shape=jax.ShapeDtypeStruct(shape, jnp.bfloat16), out_specs=HBM
    )()

    def one_round(carry):
        turn, spill = carry
        mine = pack(EXTRA, pos, CAPACITY + turn * EXTRA, table, blocks)
        got = lax.all_gather(mine, "layer")
        got = jnp.stack([got, other_core(got)])
        return turn + 1, lax.dynamic_update_slice(spill, got, (0, 0, turn * EXTRA * SUB, 0))

    return lax.while_loop(lambda carry: carry[0] < rounds, one_round, (jnp.int32(0), empty))[1]


def steps(pos, pat, current, table, most):
    f32 = jax.ShapeDtypeStruct((SHARE, WIDTH), jnp.float32)
    bf16 = jax.ShapeDtypeStruct((SHARE, WIDTH), jnp.bfloat16)
    panel_shape = jax.ShapeDtypeStruct((ORDER + SUB, WIDTH), jnp.bfloat16)
    total = pltpu.VMEM((SHARE, WIDTH), jnp.float32)
    more = pltpu.VMEM((ROUNDS * EXTRA * SUB, TILE), jnp.bfloat16)
    split = SPLIT * SUB

    def step(carry):
        turn, current = carry[:2]
        blocks = [current, along_y(current, -1), along_y(current, 2), along_y(current, 1)]
        blocks += map(other_core, blocks[:4])
        packed = pack(CAPACITY, pos, 0, table, blocks)
        spill = spilled(pos, most, table, blocks)
        turn, current, packed, spill = lax.optimization_barrier((turn + 1, current, packed, spill))
        left = whole_rows(current)
        down, up = along_z(packed, 1), along_z(packed, -1)
        down2, up2 = along_z(down, 1), along_z(up, -1)
        down2, up2, *left = lax.optimization_barrier((down2, up2, *left))
        down3, up3 = along_z(down2, 1), along_z(up2, -1)
        near = [both for one in (packed, down, up, down2, up2) for both in (one, other_core(one))]
        panel = call(near_kernel, panel_shape, 2, pos, table, *near, flops=10**9)
        down3, up3, panel = lax.optimization_barrier((down3, up3, panel))
        first_part = jax.ShapeDtypeStruct((split, TILE), jnp.bfloat16)
        last_part = jax.ShapeDtypeStruct((CAPACITY * SUB - split, TILE), jnp.bfloat16)
        part_a, part_b = call(parts_kernel, (first_part, last_part), 0, down3, up3)
        far_a, far_b = along_z(part_a, 1), along_z(part_b, -1)
        far = [both for one in (down3, up3, far_a, far_b) for both in (one, other_core(one))]
        square, square_half, panel = call(
            square_kernel,
            (f32, bf16, panel_shape),
            3,
            *(pos, pat, table, *far, panel, *left, spill),
            scratch=(total, more),
            n_hbm=1,
            aliases={11: 2},
            flops=10**9,
        )
        left = whole_rows(square_half)
        result, following = call(
            cube_kernel,
            (f32, bf16),
            2,
            *(pos, pat, square, panel, *left),
            scratch=(total,),
            flops=10**9,
        )
        return turn, following, result

    first = (jnp.int32(0), current, jnp.zeros((SHARE, WIDTH), jnp.float32))
    return lax.while_loop(lambda carry: carry[0] < STEPS, step, first)[2]


def shards(hamiltonian, tile_pattern, n_occ, mu, gamma):
    row, x, z = lax.axis_index("row"), lax.axis_index("col"), lax.axis_index("layer")
    pos = jnp.stack([row // 2, row % 2, x, z]).astype(jnp.int32)
    share = jax.ShapeDtypeStruct((SHARE, WIDTH), jnp.bfloat16)
    current = call(start_kernel, share, 5, pos, tile_pattern, n_occ, mu, gamma, hamiltonian)
    table, most = pl.pallas_call(
        table_kernel,
        out_shape=(
            jax.ShapeDtypeStruct((NZ + 1, SLOTS), jnp.int32),
            jax.ShapeDtypeStruct((1,), jnp.int32),
        ),
        in_specs=[SMEM, VMEM],
        out_specs=[VMEM, SMEM],
        compiler_params=PARAMS,
    )(pos, tile_pattern)
    return steps(pos, tile_pattern, current, table, most)


def solution(mesh):
    placed = (P(("row", "layer"), "col"), P(), P(), P(), P())
    return jax.shard_map(
        shards, mesh=mesh, in_specs=placed, out_specs=P(("row", "layer"), "col"), check_vma=False
    )
```

```python
import functools

import jax
import jax.numpy as jnp
from jax import lax
from jax.experimental import pallas as pl
from jax.experimental.pallas import tpu as pltpu
from jax.sharding import PartitionSpec as P

TILE = 128
STEPS = 2
SUB = 16

SHARE = 80
NY, NX, NZ = 4, 4, 8
ROW_BLOCK = SHARE * NZ
BAND_TILES = 10
WIDTH = BAND_TILES * TILE
TILES = 40
ORDER = TILES * TILE
NSUB = SHARE // SUB
ALL_SLOTS = 2 * NY * NSUB * BAND_TILES
Z_ORDER = (0, -1, 1, -2, 2, -3, 3, 4)
SLOTS = 512
UNROLL = 8
CAPACITY = 88
SPLIT = 48
EXTRA = 16
ROUNDS = -(-(ALL_SLOTS // 2 - CAPACITY) // EXTRA)

SMEM = pl.BlockSpec(memory_space=pltpu.SMEM)
VMEM = pl.BlockSpec(memory_space=pltpu.VMEM)
HBM = pl.BlockSpec(memory_space=pltpu.HBM)
PARAMS = pltpu.CompilerParams(vmem_limit_bytes=20 * 1024 * 1024)


def row_of(block, z, sub):
    return block * ROW_BLOCK + SHARE * z + SUB * sub


def where_am_i(pos):
    return pos[0], pos[1], pos[2], pos[3]


def start_kernel(pos, pat, n_occ, mu, gamma, hamiltonian, out):
    y, core, x, z = where_am_i(pos)
    filling = jnp.full((SUB, TILE), n_occ[0].astype(jnp.float32)) / ORDER
    apart = lax.broadcasted_iota(jnp.int32, (SUB, TILE), 1) - lax.broadcasted_iota(
        jnp.int32, (SUB, TILE), 0
    )

    def strip(s, _):
        g = row_of(2 * y + core, z, s)
        i = g // TILE
        near = apart == g % TILE
        rows = pl.ds(pl.multiple_of(s * SUB, SUB), SUB)
        for t in range(BAND_TILES):
            j = BAND_TILES * x + t
            cols = slice(t * TILE, (t + 1) * TILE)
            identity = jnp.where(near, (i == j).astype(jnp.float32), 0.0)
            h = hamiltonian[rows, cols].astype(jnp.float32)
            value = filling * identity + gamma[0] * (mu[0] * identity - h)
            out[rows, cols] = (value * pat[i, j].astype(jnp.float32)).astype(jnp.bfloat16)
        return 0

    lax.fori_loop(0, NSUB, strip, 0)


def table_kernel(pos, pat, table, most):
    y, core, x, z = where_am_i(pos)
    f32 = jnp.float32
    pattern = pat[...].astype(f32)
    n = 8 * NSUB

    def iota(shape, dim):
        return lax.broadcasted_iota(jnp.int32, shape, dim)

    rows = iota((NZ * n, TILES), 0)
    rz, rn = rows // n, rows % n
    rk = row_of(rn // NSUB, rz, rn % NSUB) // TILE
    picked = jnp.dot((rk == iota((NZ * n, TILES), 1)).astype(f32), pattern)
    total = jnp.dot(
        (iota((NZ, NZ * n), 0) == iota((NZ, NZ * n), 1) // n).astype(f32), picked
    )
    k, band = iota((TILES, NX), 0), iota((TILES, NX), 1)
    group = (k // BAND_TILES == band).astype(f32)
    most[0] = jnp.max(jnp.dot(total, group)).astype(jnp.int32)

    cols = (iota((TILES, TILE), 0) == BAND_TILES * x + iota((TILES, TILE), 1)) & (
        iota((TILES, TILE), 1) < BAND_TILES
    )
    mine = jnp.dot(pattern, cols.astype(f32))
    before = (iota((TILE, TILE), 0) < iota((TILE, TILE), 1)).astype(f32)
    below = (iota((n, n), 1) < iota((n, n), 0)).astype(f32)
    slots = iota((n, SLOTS), 1)
    for m, rel in enumerate(Z_ORDER):
        zz = (z + rel) % NZ

        def first_row(shape, dim):
            r = iota(shape, dim)
            return row_of((2 * y + r // NSUB) % (2 * NY), zz, r % NSUB)

        pick = (first_row((n, TILES), 0) // TILE == iota((n, TILES), 1)).astype(f32)
        p = jnp.dot(pick, mine)
        count = jnp.sum(p, axis=1, keepdims=True)
        ahead = jnp.sum(below * jnp.reshape(jnp.dot(pick, mine).sum(axis=1), (1, n)), axis=1, keepdims=True)
        slot = (ahead + jnp.dot(p, before)).astype(jnp.int32)
        g = first_row((n, 1), 0)
        kk = g // TILE
        kx, kt = kk // BAND_TILES, kk % BAND_TILES
        place = (kx + NX - x) % NX * BAND_TILES + kt
        to = (place * TILE + g % TILE) * 16
        r = iota((n, 1), 0)
        frm = (r // NSUB * SHARE + r % NSUB * SUB) * 16
        codes = jnp.zeros((n, SLOTS), jnp.int32)
        sources = jnp.zeros((n, SLOTS), jnp.int32)
        for t in range(BAND_TILES):
            here = (slots == slot[:, t : t + 1]) & (p[:, t : t + 1] > 0)
            codes += jnp.where(here, to + t, 0)
            if m == 0:
                sources += jnp.where(here, frm + t, 0)
        number = jnp.sum(count).astype(jnp.int32)
        at = iota((1, SLOTS), 1)
        line = jnp.sum(codes, axis=0, keepdims=True)
        line = jnp.where(at < number, line, ORDER * 16)
        table[m : m + 1, :] = jnp.where(at == SLOTS - 1, number, line)
        if m == 0:
            table[NZ : NZ + 1, :] = jnp.sum(sources, axis=0, keepdims=True)


def pack_kernel(count, pos, base, table, *refs):
    blocks, (out, block) = refs[:8], refs[8:]
    core = pos[1]
    for d, ref in enumerate(blocks):
        at = d % NY * 2 + (core if d < NY else 1 - core)
        block[pl.ds(pl.multiple_of(at * SHARE, SHARE), SHARE), :] = ref[...]

    def some(i, _):
        for u in range(UNROLL):
            slot = i * UNROLL + u
            code = table[NZ, 2 * (base[0] + slot) + core]
            row = pl.multiple_of(code // 16, SUB)
            col = pl.multiple_of(code % 16 * TILE, TILE)
            to = pl.multiple_of(slot * SUB, SUB)
            out[pl.ds(to, SUB), :] = block[pl.ds(row, SUB), pl.ds(col, TILE)]
        return 0

    lax.fori_loop(0, count // UNROLL, some, 0)


def place(table, m, core, source, panel, first, last):
    def some(i, _):
        for u in range(UNROLL):
            slot = first + i * UNROLL + u
            code = table[m, 2 * slot + core]
            row = pl.multiple_of(code // 16, SUB)
            col = pl.multiple_of(code % 16 * TILE, TILE)
            frm = pl.multiple_of((i * UNROLL + u) * SUB, SUB)
            panel[pl.ds(row, SUB), pl.ds(col, TILE)] = source[pl.ds(frm, SUB), :]
        return 0

    number = jnp.clip((table[m, SLOTS - 1] + 1 - core) // 2 - first, 0, last - first)
    lax.fori_loop(0, (number + UNROLL - 1) // UNROLL, some, 0)


def product(left, panel):
    total = None
    for m, ref in enumerate(left):
        at = slice(m * WIDTH, (m + 1) * WIDTH)
        one = jnp.dot(ref[...], panel[at, :], preferred_element_type=jnp.float32)
        total = one if total is None else total + one
    return total


def each_tile(pos, pat, use):
    y, core, x, z = where_am_i(pos)

    def strip(s, _):
        i = row_of(2 * y + core, z, s) // TILE
        rows = pl.ds(pl.multiple_of(s * SUB, SUB), SUB)
        for t in range(BAND_TILES):
            where = (rows, slice(t * TILE, (t + 1) * TILE))
            use(where, pat[i, BAND_TILES * x + t].astype(jnp.float32))
        return 0

    lax.fori_loop(0, NSUB, strip, 0)


def parts_kernel(down, up, first, last):
    first[...] = down[: SPLIT * SUB, :]
    last[...] = up[SPLIT * SUB :, :]


def near_kernel(pos, table, *refs):
    packed, panel = refs[:-1], refs[-1]
    panel[...] = jnp.zeros_like(panel)
    for q, ref in enumerate(packed):
        core = pos[1] if q % 2 == 0 else 1 - pos[1]
        place(table, q // 2, core, ref, panel, 0, CAPACITY)


def third_kernel(pos, table, *refs):
    packed, panel = refs[:4], refs[5]
    for q, ref in enumerate(packed):
        core = pos[1] if q % 2 == 0 else 1 - pos[1]
        place(table, 5 + q // 2, core, ref, panel, 0, CAPACITY)


def square_kernel(pos, pat, table, *refs):
    packed, left, spill = refs[:4], refs[5:9], refs[9]
    (square, square_half, panel), (total, more) = refs[10:13], refs[13:]
    for q, ref in enumerate(packed):
        core = pos[1] if q % 2 == 0 else 1 - pos[1]
        first, last = ((0, SPLIT), (SPLIT, CAPACITY))[q // 2]
        place(table, NZ - 1, core, ref, panel, first, last)
    for m in range(NZ):

        @pl.when(table[m, SLOTS - 1] > 2 * CAPACITY)
        def _():
            for side in range(2):
                core = pos[1] if side == 0 else 1 - pos[1]
                pltpu.sync_copy(spill.at[side, (pos[3] + Z_ORDER[m] + NZ) % NZ], more)
                place(table, m, core, more, panel, CAPACITY, CAPACITY + ROUNDS * EXTRA)

    total[...] = product(left, panel)

    def use(where, mask):
        value = total[where] * mask
        square[where] = value
        square_half[where] = value.astype(jnp.bfloat16)

    each_tile(pos, pat, use)


def cube_kernel(pos, pat, square, panel, *refs):
    left, (out, out_half), total = refs[:4], refs[4:6], refs[6]
    total[...] = product(left, panel)

    def use(where, mask):
        value = 3.0 * square[where] - 2.0 * (total[where] * mask)
        out[where] = value
        out_half[where] = value.astype(jnp.bfloat16)

    each_tile(pos, pat, use)


def ring(axis, shift, size, stride=1):
    return [(i, (i + shift * stride) % size) for i in range(size)]


def along_x(value, shift):
    return lax.ppermute(value, "col", ring("col", shift, NX))


def along_y(value, shift):
    return lax.ppermute(value, "row", ring("row", shift, 2 * NY, 2))


def along_z(value, shift):
    return lax.ppermute(value, "layer", ring("layer", shift, NZ))


def other_core(value):
    return lax.ppermute(value, "row", [(i, i ^ 1) for i in range(2 * NY)])


def whole_rows(mine):
    return [mine, along_x(mine, -1), along_x(mine, 2), along_x(mine, 1)]


def call(kernel, outs, n_smem, *args, scratch=(), n_hbm=0, flops=0, aliases=None):
    single = not isinstance(outs, (tuple, list))
    return pl.pallas_call(
        kernel,
        out_shape=outs,
        in_specs=[SMEM] * n_smem + [VMEM] * (len(args) - n_smem - n_hbm) + [HBM] * n_hbm,
        out_specs=VMEM if single else [VMEM] * len(outs),
        scratch_shapes=scratch,
        input_output_aliases=aliases or {},
        compiler_params=PARAMS,
        cost_estimate=pl.CostEstimate(flops=flops, bytes_accessed=0, transcendentals=0),
    )(*args)


def pack(count, pos, base, table, blocks):
    return call(
        functools.partial(pack_kernel, count),
        jax.ShapeDtypeStruct((count * SUB, TILE), jnp.bfloat16),
        3,
        *(pos, jnp.asarray(base, jnp.int32).reshape(1), table, *blocks),
        scratch=(pltpu.VMEM((ROW_BLOCK, WIDTH), jnp.bfloat16),),
    )


def nothing_kernel(out):
    pass


def tables(pos, pat):
    return pl.pallas_call(
        table_kernel,
        out_shape=(
            jax.ShapeDtypeStruct((NZ + 1, SLOTS), jnp.int32),
            jax.ShapeDtypeStruct((1,), jnp.int32),
        ),
        in_specs=[SMEM, VMEM],
        out_specs=[VMEM, SMEM],
        compiler_params=PARAMS,
        cost_estimate=pl.CostEstimate(flops=10**9, bytes_accessed=0, transcendentals=0),
    )(pos, pat)


def unset(shape, dtype):
    return pl.pallas_call(
        nothing_kernel, out_shape=jax.ShapeDtypeStruct(shape, dtype), out_specs=HBM
    )()


def spilled(pos, most, table, blocks):
    rounds = (most[0] - 2 * CAPACITY + 2 * EXTRA - 1) // (2 * EXTRA)
    shape = (2, NZ, ROUNDS * EXTRA * SUB, TILE)
    empty = unset(shape, jnp.bfloat16)

    def one_round(carry):
        turn, spill = carry
        mine = pack(EXTRA, pos, CAPACITY + turn * EXTRA, table, blocks)
        got = lax.all_gather(mine, "layer")
        got = jnp.stack([got, other_core(got)])
        return turn + 1, lax.dynamic_update_slice(spill, got, (0, 0, turn * EXTRA * SUB, 0))

    return lax.while_loop(lambda carry: carry[0] < rounds, one_round, (jnp.int32(0), empty))[1]


def steps(pos, pat, current):
    f32 = jax.ShapeDtypeStruct((SHARE, WIDTH), jnp.float32)
    bf16 = jax.ShapeDtypeStruct((SHARE, WIDTH), jnp.bfloat16)
    panel_shape = jax.ShapeDtypeStruct((ORDER + SUB, WIDTH), jnp.bfloat16)
    total = pltpu.VMEM((SHARE, WIDTH), jnp.float32)
    more = pltpu.VMEM((ROUNDS * EXTRA * SUB, TILE), jnp.bfloat16)
    split = SPLIT * SUB

    def step(carry):
        turn, current = carry[:2]
        blocks = [current, along_y(current, -1), along_y(current, 2), along_y(current, 1)]
        here, _ = lax.optimization_barrier((pos, current))
        table, most, *blocks = lax.optimization_barrier((*tables(here, pat), *blocks))
        blocks += map(other_core, blocks[:4])
        packed = pack(CAPACITY, pos, 0, table, blocks)
        spill = spilled(pos, most, table, blocks)
        turn, current, packed, spill = lax.optimization_barrier((turn + 1, current, packed, spill))
        left = whole_rows(current)
        down, up = along_z(packed, 1), along_z(packed, -1)
        down2, up2 = along_z(down, 1), along_z(up, -1)
        down2, up2, *left = lax.optimization_barrier((down2, up2, *left))
        down3, up3 = along_z(down2, 1), along_z(up2, -1)
        near = [both for one in (packed, down, up, down2, up2) for both in (one, other_core(one))]
        panel = call(near_kernel, panel_shape, 2, pos, table, *near, flops=10**9)
        down3, up3, panel = lax.optimization_barrier((down3, up3, panel))
        first_part = jax.ShapeDtypeStruct((split, TILE), jnp.bfloat16)
        last_part = jax.ShapeDtypeStruct((CAPACITY * SUB - split, TILE), jnp.bfloat16)
        part_a, part_b = call(parts_kernel, (first_part, last_part), 0, down3, up3)
        far_a, far_b = along_z(part_a, 1), along_z(part_b, -1)
        third = [both for one in (down3, up3) for both in (one, other_core(one))]
        panel = call(
            third_kernel, panel_shape, 2, pos, table, *third, panel, aliases={6: 0}, flops=10**9
        )
        far_a, far_b, panel = lax.optimization_barrier((far_a, far_b, panel))
        far = [both for one in (far_a, far_b) for both in (one, other_core(one))]
        square, square_half, panel = call(
            square_kernel,
            (f32, bf16, panel_shape),
            3,
            *(pos, pat, table, *far, panel, *left, spill),
            scratch=(total, more),
            n_hbm=1,
            aliases={7: 2},
            flops=10**9,
        )
        left = whole_rows(square_half)
        result, following = call(
            cube_kernel,
            (f32, bf16),
            2,
            *(pos, pat, square, panel, *left),
            scratch=(total,),
            flops=10**9,
        )
        return turn, following, result

    first = (jnp.int32(0), current, unset((SHARE, WIDTH), jnp.float32))
    return lax.while_loop(lambda carry: carry[0] < STEPS, step, first)[2]


def shards(hamiltonian, tile_pattern, n_occ, mu, gamma):
    row, x, z = lax.axis_index("row"), lax.axis_index("col"), lax.axis_index("layer")
    pos = jnp.stack([row // 2, row % 2, x, z]).astype(jnp.int32)
    share = jax.ShapeDtypeStruct((SHARE, WIDTH), jnp.bfloat16)
    current = call(start_kernel, share, 5, pos, tile_pattern, n_occ, mu, gamma, hamiltonian)
    return steps(pos, tile_pattern, current)


def solution(mesh):
    placed = (P(("row", "layer"), "col"), P(), P(), P(), P())
    return jax.shard_map(
        shards, mesh=mesh, in_specs=placed, out_specs=P(("row", "layer"), "col"), check_vma=False
    )
```

```python
import functools

import jax
import jax.numpy as jnp
from jax import lax
from jax.experimental import pallas as pl
from jax.experimental.pallas import tpu as pltpu
from jax.sharding import PartitionSpec as P

TILE = 128
STEPS = 2
SUB = 16

SHARE = 80
NY, NX, NZ = 4, 4, 8
ROW_BLOCK = SHARE * NZ
BAND_TILES = 10
WIDTH = BAND_TILES * TILE
TILES = 40
ORDER = TILES * TILE
NSUB = SHARE // SUB
ALL_SLOTS = 2 * NY * NSUB * BAND_TILES
Z_ORDER = (0, -1, 1, -2, 2, -3, 3, 4)
SLOTS = 512
UNROLL = 8
CAPACITY = 80
SPLIT = 40
EXTRA = 16
ROUNDS = -(-(ALL_SLOTS // 2 - CAPACITY) // EXTRA)

SMEM = pl.BlockSpec(memory_space=pltpu.SMEM)
VMEM = pl.BlockSpec(memory_space=pltpu.VMEM)
HBM = pl.BlockSpec(memory_space=pltpu.HBM)
PARAMS = pltpu.CompilerParams(vmem_limit_bytes=20 * 1024 * 1024)


def row_of(block, z, sub):
    return block * ROW_BLOCK + SHARE * z + SUB * sub


def where_am_i(pos):
    return pos[0], pos[1], pos[2], pos[3]


def start_kernel(pos, pat, n_occ, mu, gamma, hamiltonian, out):
    y, core, x, z = where_am_i(pos)
    filling = jnp.full((SUB, TILE), n_occ[0].astype(jnp.float32)) / ORDER
    apart = lax.broadcasted_iota(jnp.int32, (SUB, TILE), 1) - lax.broadcasted_iota(
        jnp.int32, (SUB, TILE), 0
    )

    def strip(s, _):
        g = row_of(2 * y + core, z, s)
        i = g // TILE
        near = apart == g % TILE
        rows = pl.ds(pl.multiple_of(s * SUB, SUB), SUB)
        for t in range(BAND_TILES):
            j = BAND_TILES * x + t
            cols = slice(t * TILE, (t + 1) * TILE)
            identity = jnp.where(near, (i == j).astype(jnp.float32), 0.0)
            h = hamiltonian[rows, cols].astype(jnp.float32)
            value = filling * identity + gamma[0] * (mu[0] * identity - h)
            out[rows, cols] = (value * pat[i, j].astype(jnp.float32)).astype(jnp.bfloat16)
        return 0

    lax.fori_loop(0, NSUB, strip, 0)


def table_kernel(pos, pat, table, most):
    y, core, x, z = where_am_i(pos)
    f32 = jnp.float32
    pattern = pat[...].astype(f32)
    n = 8 * NSUB

    def iota(shape, dim):
        return lax.broadcasted_iota(jnp.int32, shape, dim)

    rows = iota((NZ * n, TILES), 0)
    rz, rn = rows // n, rows % n
    rk = row_of(rn // NSUB, rz, rn % NSUB) // TILE
    picked = jnp.dot((rk == iota((NZ * n, TILES), 1)).astype(f32), pattern)
    total = jnp.dot(
        (iota((NZ, NZ * n), 0) == iota((NZ, NZ * n), 1) // n).astype(f32), picked
    )
    k, band = iota((TILES, NX), 0), iota((TILES, NX), 1)
    group = (k // BAND_TILES == band).astype(f32)
    most[0] = jnp.max(jnp.dot(total, group)).astype(jnp.int32)

    cols = (iota((TILES, TILE), 0) == BAND_TILES * x + iota((TILES, TILE), 1)) & (
        iota((TILES, TILE), 1) < BAND_TILES
    )
    mine = jnp.dot(pattern, cols.astype(f32))
    before = (iota((TILE, TILE), 0) < iota((TILE, TILE), 1)).astype(f32)
    below = (iota((n, n), 1) < iota((n, n), 0)).astype(f32)
    slots = iota((n, SLOTS), 1)
    for m, rel in enumerate(Z_ORDER):
        zz = (z + rel) % NZ

        def first_row(shape, dim):
            r = iota(shape, dim)
            return row_of((2 * y + r // NSUB) % (2 * NY), zz, r % NSUB)

        pick = (first_row((n, TILES), 0) // TILE == iota((n, TILES), 1)).astype(f32)
        p = jnp.dot(pick, mine)
        count = jnp.sum(p, axis=1, keepdims=True)
        ahead = jnp.sum(below * jnp.reshape(jnp.dot(pick, mine).sum(axis=1), (1, n)), axis=1, keepdims=True)
        slot = (ahead + jnp.dot(p, before)).astype(jnp.int32)
        g = first_row((n, 1), 0)
        kk = g // TILE
        kx, kt = kk // BAND_TILES, kk % BAND_TILES
        place = (kx + NX - x) % NX * BAND_TILES + kt
        to = (place * TILE + g % TILE) * 16
        r = iota((n, 1), 0)
        frm = (r // NSUB * SHARE + r % NSUB * SUB) * 16
        codes = jnp.zeros((n, SLOTS), jnp.int32)
        sources = jnp.zeros((n, SLOTS), jnp.int32)
        for t in range(BAND_TILES):
            here = (slots == slot[:, t : t + 1]) & (p[:, t : t + 1] > 0)
            codes += jnp.where(here, to + t, 0)
            if m == 0:
                sources += jnp.where(here, frm + t, 0)
        number = jnp.sum(count).astype(jnp.int32)
        at = iota((1, SLOTS), 1)
        line = jnp.sum(codes, axis=0, keepdims=True)
        line = jnp.where(at < number, line, ORDER * 16)
        table[m : m + 1, :] = jnp.where(at == SLOTS - 1, number, line)
        if m == 0:
            table[NZ : NZ + 1, :] = jnp.sum(sources, axis=0, keepdims=True)


def pack_kernel(count, pos, base, table, *refs):
    blocks, (out, block) = refs[:8], refs[8:]
    core = pos[1]
    for d, ref in enumerate(blocks):
        at = d % NY * 2 + (core if d < NY else 1 - core)
        block[pl.ds(pl.multiple_of(at * SHARE, SHARE), SHARE), :] = ref[...]

    def some(i, _):
        for u in range(UNROLL):
            slot = i * UNROLL + u
            code = table[NZ, 2 * (base[0] + slot) + core]
            row = pl.multiple_of(code // 16, SUB)
            col = pl.multiple_of(code % 16 * TILE, TILE)
            to = pl.multiple_of(slot * SUB, SUB)
            out[pl.ds(to, SUB), :] = block[pl.ds(row, SUB), pl.ds(col, TILE)]
        return 0

    lax.fori_loop(0, count // UNROLL, some, 0)


def place(table, m, core, source, panel, first, last):
    def some(i, _):
        for u in range(UNROLL):
            slot = first + i * UNROLL + u
            code = table[m, 2 * slot + core]
            row = pl.multiple_of(code // 16, SUB)
            col = pl.multiple_of(code % 16 * TILE, TILE)
            frm = pl.multiple_of((i * UNROLL + u) * SUB, SUB)
            panel[pl.ds(row, SUB), pl.ds(col, TILE)] = source[pl.ds(frm, SUB), :]
        return 0

    number = jnp.clip((table[m, SLOTS - 1] + 1 - core) // 2 - first, 0, last - first)
    lax.fori_loop(0, (number + UNROLL - 1) // UNROLL, some, 0)


def product(left, panel):
    total = None
    for m, ref in enumerate(left):
        at = slice(m * WIDTH, (m + 1) * WIDTH)
        one = jnp.dot(ref[...], panel[at, :], preferred_element_type=jnp.float32)
        total = one if total is None else total + one
    return total


def each_tile(pos, pat, use):
    y, core, x, z = where_am_i(pos)

    def strip(s, _):
        i = row_of(2 * y + core, z, s) // TILE
        rows = pl.ds(pl.multiple_of(s * SUB, SUB), SUB)
        for t in range(BAND_TILES):
            where = (rows, slice(t * TILE, (t + 1) * TILE))
            use(where, pat[i, BAND_TILES * x + t].astype(jnp.float32))
        return 0

    lax.fori_loop(0, NSUB, strip, 0)


def parts_kernel(down, up, first, last):
    first[...] = down[: SPLIT * SUB, :]
    last[...] = up[SPLIT * SUB :, :]


def near_kernel(pos, table, *refs):
    packed, panel = refs[:-1], refs[-1]
    panel[...] = jnp.zeros_like(panel)
    for q, ref in enumerate(packed):
        core = pos[1] if q % 2 == 0 else 1 - pos[1]
        place(table, q // 2, core, ref, panel, 0, CAPACITY)


def third_kernel(pos, table, *refs):
    packed, panel = refs[:4], refs[5]
    for q, ref in enumerate(packed):
        core = pos[1] if q % 2 == 0 else 1 - pos[1]
        place(table, 5 + q // 2, core, ref, panel, 0, CAPACITY)


def square_kernel(pos, pat, table, *refs):
    packed, left, spill = refs[:4], refs[5:9], refs[9]
    (square, square_half, panel), (total, more) = refs[10:13], refs[13:]
    for q, ref in enumerate(packed):
        core = pos[1] if q % 2 == 0 else 1 - pos[1]
        first, last = ((0, SPLIT), (SPLIT, CAPACITY))[q // 2]
        place(table, NZ - 1, core, ref, panel, first, last)
    for m in range(NZ):

        @pl.when(table[m, SLOTS - 1] > 2 * CAPACITY)
        def _():
            for side in range(2):
                core = pos[1] if side == 0 else 1 - pos[1]
                pltpu.sync_copy(spill.at[side, (pos[3] + Z_ORDER[m] + NZ) % NZ], more)
                place(table, m, core, more, panel, CAPACITY, CAPACITY + ROUNDS * EXTRA)

    total[...] = product(left, panel)

    def use(where, mask):
        value = total[where] * mask
        square[where] = value
        square_half[where] = value.astype(jnp.bfloat16)

    each_tile(pos, pat, use)


def cube_kernel(pos, pat, square, panel, *refs):
    left, (out, out_half), total = refs[:4], refs[4:6], refs[6]
    total[...] = product(left, panel)

    def use(where, mask):
        value = 3.0 * square[where] - 2.0 * (total[where] * mask)
        out[where] = value
        out_half[where] = value.astype(jnp.bfloat16)

    each_tile(pos, pat, use)


def ring(axis, shift, size, stride=1):
    return [(i, (i + shift * stride) % size) for i in range(size)]


def along_x(value, shift):
    return lax.ppermute(value, "col", ring("col", shift, NX))


def along_y(value, shift):
    return lax.ppermute(value, "row", ring("row", shift, 2 * NY, 2))


def along_z(value, shift):
    return lax.ppermute(value, "layer", ring("layer", shift, NZ))


def other_core(value):
    return lax.ppermute(value, "row", [(i, i ^ 1) for i in range(2 * NY)])


def whole_rows(mine):
    return [mine, along_x(mine, -1), along_x(mine, 2), along_x(mine, 1)]


def call(kernel, outs, n_smem, *args, scratch=(), n_hbm=0, flops=0, aliases=None):
    single = not isinstance(outs, (tuple, list))
    return pl.pallas_call(
        kernel,
        out_shape=outs,
        in_specs=[SMEM] * n_smem + [VMEM] * (len(args) - n_smem - n_hbm) + [HBM] * n_hbm,
        out_specs=VMEM if single else [VMEM] * len(outs),
        scratch_shapes=scratch,
        input_output_aliases=aliases or {},
        compiler_params=PARAMS,
        cost_estimate=pl.CostEstimate(flops=flops, bytes_accessed=0, transcendentals=0),
    )(*args)


def pack(count, pos, base, table, blocks):
    return call(
        functools.partial(pack_kernel, count),
        jax.ShapeDtypeStruct((count * SUB, TILE), jnp.bfloat16),
        3,
        *(pos, jnp.asarray(base, jnp.int32).reshape(1), table, *blocks),
        scratch=(pltpu.VMEM((ROW_BLOCK, WIDTH), jnp.bfloat16),),
    )


def nothing_kernel(out):
    pass


def tables(pos, pat):
    return pl.pallas_call(
        table_kernel,
        out_shape=(
            jax.ShapeDtypeStruct((NZ + 1, SLOTS), jnp.int32),
            jax.ShapeDtypeStruct((1,), jnp.int32),
        ),
        in_specs=[SMEM, VMEM],
        out_specs=[VMEM, SMEM],
        compiler_params=PARAMS,
        cost_estimate=pl.CostEstimate(flops=10**9, bytes_accessed=0, transcendentals=0),
    )(pos, pat)


def unset(shape, dtype):
    return pl.pallas_call(
        nothing_kernel, out_shape=jax.ShapeDtypeStruct(shape, dtype), out_specs=HBM
    )()


def spilled(pos, most, table, blocks):
    rounds = (most[0] - 2 * CAPACITY + 2 * EXTRA - 1) // (2 * EXTRA)
    shape = (2, NZ, ROUNDS * EXTRA * SUB, TILE)
    empty = unset(shape, jnp.bfloat16)

    def one_round(carry):
        turn, spill = carry
        mine = pack(EXTRA, pos, CAPACITY + turn * EXTRA, table, blocks)
        got = lax.all_gather(mine, "layer")
        got = jnp.stack([got, other_core(got)])
        return turn + 1, lax.dynamic_update_slice(spill, got, (0, 0, turn * EXTRA * SUB, 0))

    return lax.while_loop(lambda carry: carry[0] < rounds, one_round, (jnp.int32(0), empty))[1]


def steps(pos, pat, current):
    f32 = jax.ShapeDtypeStruct((SHARE, WIDTH), jnp.float32)
    bf16 = jax.ShapeDtypeStruct((SHARE, WIDTH), jnp.bfloat16)
    panel_shape = jax.ShapeDtypeStruct((ORDER + SUB, WIDTH), jnp.bfloat16)
    total = pltpu.VMEM((SHARE, WIDTH), jnp.float32)
    more = pltpu.VMEM((ROUNDS * EXTRA * SUB, TILE), jnp.bfloat16)
    split = SPLIT * SUB

    def step(carry):
        turn, current = carry[:2]
        blocks = [current, along_y(current, -1), along_y(current, 2), along_y(current, 1)]
        here, _ = lax.optimization_barrier((pos, current))
        table, most, *blocks = lax.optimization_barrier((*tables(here, pat), *blocks))
        blocks += map(other_core, blocks[:4])
        packed = pack(CAPACITY, pos, 0, table, blocks)
        spill = spilled(pos, most, table, blocks)
        turn, current, packed, spill = lax.optimization_barrier((turn + 1, current, packed, spill))
        left = whole_rows(current)
        down, up = along_z(packed, 1), along_z(packed, -1)
        down2, up2 = along_z(down, 1), along_z(up, -1)
        down2, up2, *left = lax.optimization_barrier((down2, up2, *left))
        down3, up3 = along_z(down2, 1), along_z(up2, -1)
        near = [both for one in (packed, down, up, down2, up2) for both in (one, other_core(one))]
        panel = call(near_kernel, panel_shape, 2, pos, table, *near, flops=10**9)
        down3, up3, panel = lax.optimization_barrier((down3, up3, panel))
        first_part = jax.ShapeDtypeStruct((split, TILE), jnp.bfloat16)
        last_part = jax.ShapeDtypeStruct((CAPACITY * SUB - split, TILE), jnp.bfloat16)
        part_a, part_b = call(parts_kernel, (first_part, last_part), 0, down3, up3)
        far_a, far_b = along_z(part_a, 1), along_z(part_b, -1)
        third = [both for one in (down3, up3) for both in (one, other_core(one))]
        panel = call(
            third_kernel, panel_shape, 2, pos, table, *third, panel, aliases={6: 0}, flops=10**9
        )
        far_a, far_b, panel = lax.optimization_barrier((far_a, far_b, panel))
        far = [both for one in (far_a, far_b) for both in (one, other_core(one))]
        square, square_half, panel = call(
            square_kernel,
            (f32, bf16, panel_shape),
            3,
            *(pos, pat, table, *far, panel, *left, spill),
            scratch=(total, more),
            n_hbm=1,
            aliases={7: 2},
            flops=10**9,
        )
        left = whole_rows(square_half)
        result, following = call(
            cube_kernel,
            (f32, bf16),
            2,
            *(pos, pat, square, panel, *left),
            scratch=(total,),
            flops=10**9,
        )
        return turn, following, result

    first = (jnp.int32(0), current, unset((SHARE, WIDTH), jnp.float32))
    return lax.while_loop(lambda carry: carry[0] < STEPS, step, first)[2]


def shards(hamiltonian, tile_pattern, n_occ, mu, gamma):
    row, x, z = lax.axis_index("row"), lax.axis_index("col"), lax.axis_index("layer")
    pos = jnp.stack([row // 2, row % 2, x, z]).astype(jnp.int32)
    share = jax.ShapeDtypeStruct((SHARE, WIDTH), jnp.bfloat16)
    current = call(start_kernel, share, 5, pos, tile_pattern, n_occ, mu, gamma, hamiltonian)
    return steps(pos, tile_pattern, current)


def solution(mesh):
    placed = (P(("row", "layer"), "col"), P(), P(), P(), P())
    return jax.shard_map(
        shards, mesh=mesh, in_specs=placed, out_specs=P(("row", "layer"), "col"), check_vma=False
    )
```
